128 devices in a mesh: row: 8 (over z, core), col: 16 (over y, x).
Axes of the slice: x: 4, y: 4, z: 4, core: 2. Of those that a mesh axis runs over, the one named last changes fastest.
Arguments:
- features: bfloat16 [64, 524288], P(None, ('row', 'col')), may hold values from -6 to 6
- tile_rows: int32 [8, 16, 512], P('row', 'col'), may hold values from 0 to 511, as said below
- tile_cols: int32 [8, 16, 512], P('row', 'col'), may hold values from 0 to 255
- tile_count: int32 [8, 16], P('row', 'col'), may hold values from 1 to 512, as said below
- tile_data: bfloat16 [8, 16, 512, 128, 128], P('row', 'col'), may hold values from -0.21875 to 0.21875
Outputs:
- filtered: bfloat16 [512, 524288], P(None, ('row', 'col'))
The draws below stay inside these ranges and needn't reach their ends.
Inputs may be any that keep to these rules, and one draw needn't show every extreme that they name: Within one device the pairs (tile_rows, tile_cols) of all 512 slots are distinct. `tile_count`: some device has all 512 slots live in every draw.
All inputs are finite; a program needn't handle non-finite values.
Results may differ from the reference program's by a relative error of at most 0.009.
Values may be sent and summed in bfloat16 or wider, within the bound.
A program may use at most 128 MiB of HBM per device.

```python
import jax
import jax.numpy as jnp
from jax import lax

CHANNELS = 64
SCALES = 8
TILE_SIZE = 128
NODES_DEV = 4096
TILES_MAX = 512
NODES = 524288
BLOCK_ROWS = 512
N_ROW = 8
N_COL = 16


def tile_cells(key):
    row_blocks = NODES_DEV * N_COL // TILE_SIZE
    col_blocks = NODES_DEV * N_ROW // TILE_SIZE
    keys = jax.random.split(jax.random.fold_in(key, 11), N_ROW * N_COL)

    def one_device(device_key):
        return jax.random.permutation(device_key, row_blocks * col_blocks)[:TILES_MAX]
    cells = jax.vmap(one_device)(keys)
    return (cells.reshape(N_ROW, N_COL, TILES_MAX).astype(jnp.int32), col_blocks)


def draw_tile_rows(key, part):
    cells, col_blocks = tile_cells(key)
    return (cells // col_blocks).astype(jnp.int32)


def draw_tile_cols(key, part):
    cells, col_blocks = tile_cells(key)
    return (cells % col_blocks).astype(jnp.int32)


def draw_tile_count(key, part):
    device_count = N_ROW * N_COL
    base_key = jax.random.fold_in(key, 23)
    full_key = jax.random.fold_in(key, 29)
    lowest = max(1, TILES_MAX // 8)
    highest = max(lowest + 1, TILES_MAX // 2 + 1)
    counts = jax.random.randint(base_key, (device_count,), lowest, highest).astype(jnp.int32)
    chosen = jax.random.permutation(full_key, device_count)[:max(1, device_count // 16)]
    counts = counts.at[chosen].set(TILES_MAX)
    return counts.reshape(N_ROW, N_COL).astype(jnp.int32)


def levels(key, shape, pieces, least, top_value):
    loudness, own = 1.0, jax.random.fold_in(key, 6)
    for axis_at, shards_of in pieces:
        draws = jnp.exp(jax.random.uniform(jax.random.fold_in(own, axis_at), (shards_of,), jnp.float32, least / len(pieces), top_value / len(pieces)))
        loudness = loudness * jnp.repeat(draws, shape[axis_at] // shards_of).reshape([-1 if axis == axis_at else 1 for axis in range(len(shape))])
    return loudness


def centred(stream_key, shape, deviation, bound, shards=(), kind=jnp.bfloat16):
    array = jax.random.normal(stream_key, shape, jnp.float32) * deviation
    if len(shards) > 0:
        array = levels(stream_key, shape, shards, -0.22, 0.18) * array
    return jnp.clip(array, min=-bound, max=bound).astype(kind)


def setup_inputs(seed: int = 0) -> dict:
    arg_keys = jax.random.split(jax.random.key(seed), 6)
    return {
        "features": centred(arg_keys[0], (CHANNELS, NODES), 1.0, 6.0, ((1, 128),)),
        "tile_rows": draw_tile_rows(jax.random.fold_in(arg_keys[5], 71), 0),
        "tile_cols": draw_tile_cols(jax.random.fold_in(arg_keys[5], 71), 0),
        "tile_count": draw_tile_count(jax.random.fold_in(arg_keys[5], 71), 0),
        "tile_data": centred(arg_keys[4], (N_ROW, N_COL, TILES_MAX, TILE_SIZE, TILE_SIZE), 768 ** -0.5, 0.21875, ((0, 8), (1, 16))),
    }


def bessel_pair(times):
    halved = times / 2.0
    square = halved * halved
    term_zero = jnp.ones_like(times)
    term_one = halved
    sum_zero = term_zero
    sum_one = term_one
    for degree in range(1, 24):
        term_zero = term_zero * square / float(degree * degree)
        term_one = term_one * square / float(degree * (degree + 1))
        sum_zero = sum_zero + term_zero
        sum_one = sum_one + term_one
    damping = jnp.exp(-times)
    return damping * sum_zero, damping * sum_one


def coefficients():
    times = 0.25 * 2.0 ** (jnp.arange(SCALES).astype(jnp.float32) / 2.0)
    bessel_zero, bessel_one = bessel_pair(times)
    return bessel_zero, -2.0 * bessel_one, 2.0 * (bessel_zero - 2.0 * bessel_one / times)


def apply_operator(field, tile_rows, tile_cols, tile_count, tile_data):
    per_block = NODES_DEV // TILE_SIZE
    blocks = field.reshape(CHANNELS, NODES // TILE_SIZE, TILE_SIZE)
    device_count = N_ROW * N_COL
    slot_rows = tile_rows.reshape(device_count, TILES_MAX)
    slot_cols = tile_cols.reshape(device_count, TILES_MAX)
    slot_live = tile_count.reshape(device_count)
    slot_data = tile_data.reshape(device_count, TILES_MAX, TILE_SIZE, TILE_SIZE)

    def one_device(summed, inputs):
        row_ids, col_ids, live_count, entries, device = inputs
        row_group = device // N_COL
        col_group = device % N_COL
        global_cols = ((col_ids // per_block) * N_COL + col_group) * per_block + col_ids % per_block
        picked = jnp.take(blocks, global_cols.astype(jnp.int32), axis=1)
        product = jnp.einsum("fgk,grk->fgr", picked.astype(jnp.float32), entries.astype(jnp.float32))
        live = (jnp.arange(TILES_MAX) < live_count).astype(jnp.float32)
        product = product * live[None, :, None]
        partial_value = jnp.zeros((CHANNELS, BLOCK_ROWS, TILE_SIZE), jnp.float32).at[:, row_ids].add(product)
        partial_value = partial_value.astype(jnp.bfloat16).astype(jnp.float32)
        offset = (row_group * BLOCK_ROWS).astype(jnp.int32)
        current = lax.dynamic_slice_in_dim(summed, offset, BLOCK_ROWS, 1)
        summed = lax.dynamic_update_slice_in_dim(summed, current + partial_value, offset, 1)
        return summed, None

    start = jnp.zeros((CHANNELS, NODES // TILE_SIZE, TILE_SIZE), jnp.float32)
    device_ids = jnp.arange(device_count).astype(jnp.int32)
    summed, _ = lax.scan(one_device, start, (slot_rows, slot_cols, slot_live, slot_data, device_ids))
    return summed.reshape(CHANNELS, NODES).astype(jnp.bfloat16)


def reference(features, tile_rows, tile_cols, tile_count, tile_data):
    first = apply_operator(features, tile_rows, tile_cols, tile_count, tile_data)
    second = apply_operator(first, tile_rows, tile_cols, tile_count, tile_data)
    coef_zero, coef_one, coef_two = coefficients()
    base = features.astype(jnp.float32)
    first_wide = first.astype(jnp.float32)
    second_wide = second.astype(jnp.float32)
    filtered = (coef_zero[:, None, None] * base[None] + coef_one[:, None, None] * first_wide[None]
                + coef_two[:, None, None] * (2.0 * second_wide - base)[None])
    return filtered.reshape(SCALES * CHANNELS, NODES).astype(jnp.bfloat16)
```

```python
import functools

import jax
import jax.numpy as jnp
from jax import lax
from jax.experimental import pallas as pl
from jax.experimental.pallas import tpu as pltpu
from jax.sharding import PartitionSpec as P

TILE = 128
SLOTS = 512
CHANNELS = 64
CHUNKS = 2
CH = CHANNELS // CHUNKS
SCALES = 8
OWN = 32
UNROLL = 16
MESH = pl.DeviceIdType.MESH
BF = jnp.bfloat16
F32 = jnp.float32


def bessel_pair(times):
    halved = times / 2.0
    square = halved * halved
    term_zero = jnp.ones_like(times)
    term_one = halved
    sum_zero = term_zero
    sum_one = term_one
    for degree in range(1, 24):
        term_zero = term_zero * square / float(degree * degree)
        term_one = term_one * square / float(degree * (degree + 1))
        sum_zero = sum_zero + term_zero
        sum_one = sum_one + term_one
    damping = jnp.exp(-times)
    return (damping * sum_zero, damping * sum_one)


def coefficients():
    times = 0.25 * 2.0 ** (jnp.arange(SCALES).astype(jnp.float32) / 2.0)
    bessel_zero, bessel_one = bessel_pair(times)
    return (bessel_zero, -2.0 * bessel_one, 2.0 * (bessel_zero - 2.0 * bessel_one / times))


def slot_tables(slot_rows, slot_cols, live_count):
    ids = jnp.arange(SLOTS, dtype=jnp.int32)
    row = jnp.where(ids < live_count, slot_rows, SLOTS)
    key = row * SLOTS + ids
    rank = jnp.sum((key[None, :] < key[:, None]).astype(jnp.int32), axis=1)
    hit = rank[:, None] == ids[None, :]
    packed = (row * SLOTS + ids) * 256 + slot_cols
    ordered = jnp.sum(jnp.where(hit, packed[:, None], 0), axis=0)
    cols = ordered % 256
    perm = (ordered // 256) % SLOTS
    rows = ordered // (256 * SLOTS)
    before = jnp.concatenate([jnp.full((1,), -1, jnp.int32), rows[:-1]])
    keep = (rows == before).astype(F32)
    upto = jnp.sum((row[:, None] <= ids[None, :]).astype(jnp.int32), axis=0)
    here = jnp.sum((row[:, None] == ids[None, :]).astype(jnp.int32), axis=0)
    last = jnp.where(here > 0, upto - 1, SLOTS)
    return perm, cols, keep, last


def chain_kernel(
    perm, cols, keep, last, feat, tdata, first_out, second_out,
    tiles, f00, f01, f10, f11, runs, p0, p1,
    r00, r01, r10, r11, q00, q01, q10, q11,
    tile_sem, s1, v1, s2, v2, sa, va,
):
    row = lax.axis_index("row")
    col = lax.axis_index("col")
    z, core = row // 2, row % 2
    y, x = col // 4, col % 4
    fields = ((f00, f01), (f10, f11))
    parts = (p0, p1)
    recv1 = ((r00, r01), (r10, r11))
    recv2 = ((q00, q01), (q10, q11))
    outs = (first_out, second_out)

    def up(v):
        return (v + 1) % 4

    def down(v):
        return (v + 3) % 4

    def far(v):
        return (v + 2) % 4

    z_next = (up(z) * 2 + core, col)
    z_prev = (down(z) * 2 + core, col)
    mate = (z * 2 + (1 - core), col)
    x_next = (row, y * 4 + up(x))
    x_prev = (row, y * 4 + down(x))
    y_next = (row, up(y) * 4 + x)
    y_prev = (row, down(y) * 4 + x)

    barrier = pltpu.get_barrier_semaphore()
    for other in (z_next, z_prev, mate, x_next, x_prev, y_next, y_prev):
        pl.semaphore_signal(barrier, inc=1, device_id=other, device_id_type=MESH)

    tile_copy = pltpu.make_async_copy(tdata, tiles, tile_sem)
    tile_copy.start()

    def send(src, dst, ssem, rsem, to):
        return pltpu.make_async_remote_copy(
            src_ref=src, dst_ref=dst, send_sem=ssem, recv_sem=rsem,
            device_id=to, device_id_type=MESH,
        )

    def gather(a, k):
        ref = fields[a][k]
        half = OWN // 2

        def block(zz, h=None):
            start = (zz * 2 + core) * OWN
            if h is None:
                return ref.at[pl.ds(start, OWN)]
            return ref.at[pl.ds(start + h * half, half)]

        def copy(i, view, to):
            return send(view, view, sa.at[a, k, i], va.at[a, k, i], to)

        zp, zn, zf = down(z), up(z), far(z)
        return [
            copy(0, block(z, 0), z_next),
            copy(1, block(z, 1), z_next),
            copy(2, block(z, 0), z_prev),
            copy(3, block(z, 1), z_prev),
            copy(4, block(zp, 0), z_next),
            copy(5, block(zn, 1), z_prev),
            copy(6, block(z), mate),
            copy(7, block(zp, 0), mate),
            copy(8, block(zp, 1), mate),
            copy(9, block(zn, 0), mate),
            copy(10, block(zn, 1), mate),
            copy(11, block(zf, 0), mate),
            copy(12, block(zf, 1), mate),
        ]

    def gather_start(g):
        g[0].start()
        g[3].start()
        g[1].start()
        g[2].start()
        g[6].start()

    def gather_relay(g):
        g[0].wait_recv()
        g[4].start()
        g[7].start()
        g[3].wait_recv()
        g[5].start()
        g[10].start()

    def gather_finish(g):
        g[1].wait_recv()
        g[8].start()
        g[2].wait_recv()
        g[9].start()
        g[4].wait_recv()
        g[11].start()
        g[5].wait_recv()
        g[12].start()
        for i in range(6, 13):
            g[i].wait_recv()

    def gather_sent(g):
        for c in g:
            c.wait_send()

    def products(a, k, begin, end, acc):
        field = fields[a][k]

        def trip(i, acc):
            for u in range(UNROLL):
                s = i * UNROLL + u
                product = lax.dot_general(
                    field[cols[s]], tiles[perm[s]], (((1,), (1,)), ((), ())),
                    preferred_element_type=F32,
                )
                acc = acc * keep[s] + product
                runs[s] = acc.astype(BF)
            return acc

        return lax.fori_loop(begin // UNROLL, end // UNROLL, trip, acc)

    def zero():
        return jnp.zeros((CH, TILE), F32)

    def pack(k):
        part = parts[k]

        def trip(i, carry):
            for xx in range(4):
                for u in range(8):
                    b = (i // 4) * 128 + xx * 32 + (i % 4) * 8 + u
                    part[i // 4, xx, (i % 4) * 8 + u] = runs[last[b]]
            return carry

        lax.fori_loop(0, 16, trip, 0)

    def scatter1(a, k):
        part, got = parts[k], recv1[a][k]
        out = []
        for st in range(2):
            base = st * 16
            me = x if st == 0 else y
            nxt = x_next if st == 0 else y_next
            prv = x_prev if st == 0 else y_prev

            def view(who, h, st=st, base=base):
                if st == 0:
                    return part.at[:, who, pl.ds(base + 8 * h, 8)]
                return part.at[who, :, pl.ds(base + 8 * h, 8)]

            rows = []
            for d in range(2):
                to = nxt if d == 0 else prv
                near = up(me) if d == 0 else down(me)
                views = (view(far(me), d), view(near, 1 - d), view(near, d))
                rows.append([
                    send(views[m], got.at[st, d, m], s1.at[a, k, st, d, m], v1.at[a, k, st, d, m], to)
                    for m in range(3)
                ])
            out.append(rows)
        return out

    def scatter2(a, k):
        part, got = parts[k], recv2[a][k]
        out = []
        for st in range(2):
            base = st * 16
            me = y if st == 0 else x
            nxt = y_next if st == 0 else x_next
            prv = y_prev if st == 0 else x_prev

            def view(who, h, st=st, base=base):
                if st == 0:
                    return part.at[who, x, pl.ds(base + 8 * h, 8)]
                return part.at[y, who, pl.ds(base + 8 * h, 8)]

            rows = []
            for d in range(2):
                to = nxt if d == 0 else prv
                near = up(me) if d == 0 else down(me)
                views = (view(far(me), d), view(near, 1 - d), view(near, d))
                rows.append([
                    send(views[m], got.at[st, d, m], s2.at[a, k, st, d, m], v2.at[a, k, st, d, m], to)
                    for m in range(3)
                ])
            out.append(rows)
        return out

    def start_messages(copies, m):
        for st in range(2):
            for d in range(2):
                copies[st][d][m].start()

    def carry1(a, k, copies):
        part, got = parts[k], recv1[a][k]
        for st in range(2):
            me = x if st == 0 else y
            for d in range(2):
                near = up(me) if d == 0 else down(me)
                lo = st * 16 + 8 * d
                copies[st][d][0].wait_recv()

                def trip(i, c, st=st, d=d, near=near, lo=lo):
                    for u in range(8):
                        there = got[st, d, 0, i, u].astype(F32)
                        if st == 0:
                            mine = part[i, near, lo + u].astype(F32)
                            part[i, near, lo + u] = (mine + there).astype(BF)
                        else:
                            mine = part[near, i, lo + u].astype(F32)
                            part[near, i, lo + u] = (mine + there).astype(BF)
                    return c

                lax.fori_loop(0, 4, trip, 0)
                copies[st][d][2].start()

    def close1(a, k, copies):
        part, got = parts[k], recv1[a][k]
        for m in (1, 2):
            for st in range(2):
                for d in range(2):
                    copies[st][d][m].wait_recv()
        for st in range(2):
            for h in range(2):
                lo = st * 16 + 8 * h

                def trip(i, c, st=st, h=h, lo=lo):
                    for u in range(8):
                        total = (
                            got[st, h, 2, i, u].astype(F32) + got[st, 1 - h, 1, i, u].astype(F32)
                        )
                        if st == 0:
                            part[i, x, lo + u] = (part[i, x, lo + u].astype(F32) + total).astype(BF)
                        else:
                            part[y, i, lo + u] = (part[y, i, lo + u].astype(F32) + total).astype(BF)
                    return c

                lax.fori_loop(0, 4, trip, 0)

    def carry2(a, k, copies):
        part, got = parts[k], recv2[a][k]
        for st in range(2):
            me = y if st == 0 else x
            for d in range(2):
                near = up(me) if d == 0 else down(me)
                lo = st * 16 + 8 * d
                copies[st][d][0].wait_recv()
                for u in range(8):
                    there = got[st, d, 0, u].astype(F32)
                    if st == 0:
                        part[near, x, lo + u] = (part[near, x, lo + u].astype(F32) + there).astype(BF)
                    else:
                        part[y, near, lo + u] = (part[y, near, lo + u].astype(F32) + there).astype(BF)
                copies[st][d][2].start()

    def close2(a, k, copies):
        part, got = parts[k], recv2[a][k]
        for m in (1, 2):
            for st in range(2):
                for d in range(2):
                    copies[st][d][m].wait_recv()
        for st in range(2):
            for h in range(2):
                for u in range(8):
                    b = st * 16 + 8 * h + u
                    total = (
                        part[y, x, b].astype(F32)
                        + got[st, h, 2, u].astype(F32)
                        + got[st, 1 - h, 1, u].astype(F32)
                    ).astype(BF)
                    outs[a][k, b] = total
                    if a == 0:
                        fields[1][k][row * OWN + b] = total

    def scatter_sent(*many):
        for copies in many:
            for st in range(2):
                for d in range(2):
                    for m in range(3):
                        copies[st][d][m].wait_send()

    for k in range(CHUNKS):
        for j in range(OWN):
            fields[0][k][row * OWN + j] = feat[k * CH:(k + 1) * CH, j * TILE:(j + 1) * TILE]
    runs[SLOTS] = jnp.zeros((CH, TILE), BF)

    pl.semaphore_wait(barrier, 7)
    g = [[gather(a, k) for k in range(CHUNKS)] for a in range(2)]
    c1 = [[scatter1(a, k) for k in range(CHUNKS)] for a in range(2)]
    c2 = [[scatter2(a, k) for k in range(CHUNKS)] for a in range(2)]

    gather_start(g[0][0])
    gather_relay(g[0][0])
    gather_start(g[0][1])
    gather_finish(g[0][0])
    tile_copy.wait()

    for a in range(2):
        acc = products(a, 0, 0, SLOTS // 2, zero())
        gather_relay(g[a][1])
        products(a, 0, SLOTS // 2, SLOTS, acc)
        if a == 1:
            scatter_sent(c1[0][0], c2[0][0])
        pack(0)
        start_messages(c1[a][0], 0)
        start_messages(c1[a][0], 1)
        gather_finish(g[a][1])
        products(a, 1, 0, SLOTS, zero())
        carry1(a, 0, c1[a][0])
        if a == 1:
            scatter_sent(c1[0][1], c2[0][1])
        pack(1)
        start_messages(c1[a][1], 0)
        close1(a, 0, c1[a][0])
        start_messages(c2[a][0], 0)
        start_messages(c2[a][0], 1)
        start_messages(c1[a][1], 1)
        carry2(a, 0, c2[a][0])
        carry1(a, 1, c1[a][1])
        close2(a, 0, c2[a][0])
        if a == 0:
            gather_start(g[1][0])
        close1(a, 1, c1[a][1])
        start_messages(c2[a][1], 0)
        start_messages(c2[a][1], 1)
        if a == 0:
            gather_relay(g[1][0])
        carry2(a, 1, c2[a][1])
        if a == 0:
            gather_finish(g[1][0])
        close2(a, 1, c2[a][1])
        if a == 0:
            gather_start(g[1][1])

    for a in range(2):
        for k in range(CHUNKS):
            gather_sent(g[a][k])
    scatter_sent(c1[1][0], c2[1][0], c1[1][1], c2[1][1])


def combine_kernel(coef, feat, first, second, out):
    for k in range(CHUNKS):
        for j in range(OWN):
            nodes = slice(j * TILE, (j + 1) * TILE)
            base = feat[k * CH:(k + 1) * CH, nodes].astype(F32)
            one = first[k, j].astype(F32)
            two = 2.0 * second[k, j].astype(F32) - base
            for s in range(SCALES):
                value = coef[0, s] * base + coef[1, s] * one + coef[2, s] * two
                out[s * CHANNELS + k * CH:s * CHANNELS + (k + 1) * CH, nodes] = value.astype(BF)


def shards(features, tile_rows, tile_cols, tile_count, tile_data):
    perm, cols, keep, last = slot_tables(
        tile_rows.reshape(-1), tile_cols.reshape(-1), tile_count.reshape(())
    )
    smem = pl.BlockSpec(memory_space=pltpu.SMEM)
    vmem = pl.BlockSpec(memory_space=pltpu.VMEM)
    half = jax.ShapeDtypeStruct((CHUNKS, OWN, CH, TILE), BF)
    field = pltpu.VMEM((8 * OWN, CH, TILE), BF)
    part = pltpu.VMEM((4, 4, OWN, CH, TILE), BF)
    got1 = pltpu.VMEM((2, 2, 3, 4, 8, CH, TILE), BF)
    got2 = pltpu.VMEM((2, 2, 3, 8, CH, TILE), BF)
    dma = pltpu.SemaphoreType.DMA
    first, second = pl.pallas_call(
        chain_kernel,
        out_shape=(half, half),
        in_specs=[smem, smem, smem, smem, vmem, pl.BlockSpec(memory_space=pl.ANY)],
        out_specs=(vmem, vmem),
        scratch_shapes=[
            pltpu.VMEM((SLOTS, TILE, TILE), BF),
            field, field, field, field,
            pltpu.VMEM((SLOTS + 1, CH, TILE), BF),
            part, part,
            got1, got1, got1, got1,
            got2, got2, got2, got2,
            dma,
            dma((2, CHUNKS, 2, 2, 3)), dma((2, CHUNKS, 2, 2, 3)),
            dma((2, CHUNKS, 2, 2, 3)), dma((2, CHUNKS, 2, 2, 3)),
            dma((2, CHUNKS, 13)), dma((2, CHUNKS, 13)),
        ],
        compiler_params=pltpu.CompilerParams(
            collective_id=0, has_side_effects=True, vmem_limit_bytes=62 * 1024 * 1024
        ),
        name="chain",
    )(perm, cols, keep, last, features, tile_data.reshape(SLOTS, TILE, TILE))

    coef = jnp.stack(coefficients())
    return pl.pallas_call(
        combine_kernel,
        out_shape=jax.ShapeDtypeStruct((SCALES * CHANNELS, OWN * TILE), BF),
        in_specs=[smem, vmem, vmem, vmem],
        out_specs=vmem,
        name="combine",
    )(coef, features, first, second)


def solution(mesh):
    return jax.shard_map(
        shards,
        mesh=mesh,
        in_specs=(
            P(None, ("row", "col")),
            P("row", "col", None),
            P("row", "col", None),
            P("row", "col"),
            P("row", "col", None, None, None),
        ),
        out_specs=P(None, ("row", "col")),
        check_vma=False,
    )
```

```python
import functools

import jax
import jax.numpy as jnp
from jax import lax
from jax.experimental import pallas as pl
from jax.experimental.pallas import tpu as pltpu
from jax.sharding import PartitionSpec as P

TILE = 128
SLOTS = 512
CHANNELS = 64
CHUNKS = 4
CH = CHANNELS // CHUNKS
SCALES = 8
OWN = 32
UNROLL = 64
MESH = pl.DeviceIdType.MESH
BF = jnp.bfloat16
F32 = jnp.float32


def bessel_pair(times):
    halved = times / 2.0
    square = halved * halved
    term_zero = jnp.ones_like(times)
    term_one = halved
    sum_zero = term_zero
    sum_one = term_one
    for degree in range(1, 24):
        term_zero = term_zero * square / float(degree * degree)
        term_one = term_one * square / float(degree * (degree + 1))
        sum_zero = sum_zero + term_zero
        sum_one = sum_one + term_one
    damping = jnp.exp(-times)
    return (damping * sum_zero, damping * sum_one)


def coefficients():
    times = 0.25 * 2.0 ** (jnp.arange(SCALES).astype(jnp.float32) / 2.0)
    bessel_zero, bessel_one = bessel_pair(times)
    return (bessel_zero, -2.0 * bessel_one, 2.0 * (bessel_zero - 2.0 * bessel_one / times))


def slot_tables(slot_rows, slot_cols, live_count):
    ids = jnp.arange(SLOTS, dtype=jnp.int32)
    row = jnp.where(ids < live_count, slot_rows, SLOTS)
    key = row * SLOTS + ids
    rank = jnp.sum((key[None, :] < key[:, None]).astype(jnp.int32), axis=1)
    hit = rank[:, None] == ids[None, :]
    packed = (row * SLOTS + ids) * 256 + slot_cols
    ordered = jnp.sum(jnp.where(hit, packed[:, None], 0), axis=0)
    cols = ordered % 256
    perm = (ordered // 256) % SLOTS
    rows = ordered // (256 * SLOTS)
    before = jnp.concatenate([jnp.full((1,), -1, jnp.int32), rows[:-1]])
    keep = (rows == before).astype(F32)
    upto = jnp.sum((row[:, None] <= ids[None, :]).astype(jnp.int32), axis=0)
    here = jnp.sum((row[:, None] == ids[None, :]).astype(jnp.int32), axis=0)
    last = jnp.where(here > 0, upto - 1, SLOTS)
    return perm, cols, keep, last


def chain_kernel(
    perm, cols, keep, last, feat, tdata, first_out, second_out,
    tiles, f00, f01, f02, f03, f10, f11, f12, f13, runs, parts, recv1, recv2,
    tile_sem, s1, v1, s2, v2, sa, va,
):
    row = lax.axis_index("row")
    col = lax.axis_index("col")
    z, core = row // 2, row % 2
    y, x = col // 4, col % 4
    fields = ((f00, f01, f02, f03), (f10, f11, f12, f13))
    outs = (first_out, second_out)

    def up(v):
        return (v + 1) % 4

    def down(v):
        return (v + 3) % 4

    def far(v):
        return (v + 2) % 4

    z_next = (up(z) * 2 + core, col)
    z_prev = (down(z) * 2 + core, col)
    mate = (z * 2 + (1 - core), col)
    x_next = (row, y * 4 + up(x))
    x_prev = (row, y * 4 + down(x))
    y_next = (row, up(y) * 4 + x)
    y_prev = (row, down(y) * 4 + x)

    barrier = pltpu.get_barrier_semaphore()
    for other in (z_next, z_prev, mate, x_next, x_prev, y_next, y_prev):
        pl.semaphore_signal(barrier, inc=1, device_id=other, device_id_type=MESH)

    tile_copy = pltpu.make_async_copy(tdata, tiles, tile_sem)
    tile_copy.start()

    def send(src, dst, ssem, rsem, to):
        return pltpu.make_async_remote_copy(
            src_ref=src, dst_ref=dst, send_sem=ssem, recv_sem=rsem,
            device_id=to, device_id_type=MESH,
        )

    def gather(a, k):
        ref = fields[a][k]
        half = OWN // 2

        def block(zz, h=None):
            start = (zz * 2 + core) * OWN
            if h is None:
                return ref.at[pl.ds(start, OWN)]
            return ref.at[pl.ds(start + h * half, half)]

        def copy(i, view, to):
            return send(view, view, sa.at[a, k, i], va.at[a, k, i], to)

        zp, zn, zf = down(z), up(z), far(z)
        return [
            copy(0, block(z, 0), z_next),
            copy(1, block(z, 1), z_next),
            copy(2, block(z, 0), z_prev),
            copy(3, block(z, 1), z_prev),
            copy(4, block(zp, 0), z_next),
            copy(5, block(zn, 1), z_prev),
            copy(6, block(z), mate),
            copy(7, block(zp, 0), mate),
            copy(8, block(zp, 1), mate),
            copy(9, block(zn, 0), mate),
            copy(10, block(zn, 1), mate),
            copy(11, block(zf, 0), mate),
            copy(12, block(zf, 1), mate),
        ]

    def gather_start(g):
        g[0].start()
        g[3].start()
        g[1].start()
        g[2].start()
        g[6].start()

    def gather_relay(g):
        g[0].wait_recv()
        g[4].start()
        g[7].start()
        g[3].wait_recv()
        g[5].start()
        g[10].start()

    def gather_share(g):
        g[1].wait_recv()
        g[8].start()
        g[2].wait_recv()
        g[9].start()
        g[4].wait_recv()
        g[11].start()
        g[5].wait_recv()
        g[12].start()

    def gather_finish(g):
        for i in range(6, 13):
            g[i].wait_recv()

    def gather_sent(g):
        for c in g:
            c.wait_send()

    def products(a, k, begin, end, acc):
        field = fields[a][k]
        blank = jnp.zeros((CH, TILE), BF)

        def trip(i, acc):
            for u in range(0, UNROLL, 2):
                s = i * UNROLL + u
                lhs = jnp.concatenate([
                    jnp.concatenate([field[cols[s]], blank], axis=1),
                    jnp.concatenate([blank, field[cols[s + 1]]], axis=1),
                ], axis=0)
                rhs = jnp.concatenate([tiles[perm[s]], tiles[perm[s + 1]]], axis=1)
                pair = lax.dot_general(
                    lhs, rhs, (((1,), (1,)), ((), ())), preferred_element_type=F32
                )
                acc = acc * keep[s] + pair[:CH]
                runs[s] = acc.astype(BF)
                acc = acc * keep[s + 1] + pair[CH:]
                runs[s + 1] = acc.astype(BF)
            return acc

        return lax.fori_loop(begin // UNROLL, end // UNROLL, trip, acc)

    def zero():
        return jnp.zeros((CH, TILE), F32)

    def pack(k):
        part = parts.at[k]

        def trip(i, carry):
            for xx in range(4):
                for u in range(8):
                    b = (i // 4) * 128 + xx * 32 + (i % 4) * 8 + u
                    part[i // 4, xx, (i % 4) * 8 + u] = runs[last[b]]
            return carry

        lax.fori_loop(0, 16, trip, 0)

    def scatter1(a, k):
        part, got = parts.at[k], recv1.at[a, k]
        out = []
        for st in range(2):
            base = st * 16
            me = x if st == 0 else y
            nxt = x_next if st == 0 else y_next
            prv = x_prev if st == 0 else y_prev

            def view(who, h, st=st, base=base):
                if st == 0:
                    return part.at[:, who, pl.ds(base + 8 * h, 8)]
                return part.at[who, :, pl.ds(base + 8 * h, 8)]

            rows = []
            for d in range(2):
                to = nxt if d == 0 else prv
                near = up(me) if d == 0 else down(me)
                views = (view(far(me), d), view(near, 1 - d), view(near, d))
                rows.append([
                    send(views[m], got.at[st, d, m], s1.at[a, k, st, d, m], v1.at[a, k, st, d, m], to)
                    for m in range(3)
                ])
            out.append(rows)
        return out

    def scatter2(a, k):
        part, got = parts.at[k], recv2.at[a, k]
        out = []
        for st in range(2):
            base = st * 16
            me = y if st == 0 else x
            nxt = y_next if st == 0 else x_next
            prv = y_prev if st == 0 else x_prev

            def view(who, h, st=st, base=base):
                if st == 0:
                    return part.at[who, x, pl.ds(base + 8 * h, 8)]
                return part.at[y, who, pl.ds(base + 8 * h, 8)]

            rows = []
            for d in range(2):
                to = nxt if d == 0 else prv
                near = up(me) if d == 0 else down(me)
                views = (view(far(me), d), view(near, 1 - d), view(near, d))
                rows.append([
                    send(views[m], got.at[st, d, m], s2.at[a, k, st, d, m], v2.at[a, k, st, d, m], to)
                    for m in range(3)
                ])
            out.append(rows)
        return out

    def start_messages(copies, m):
        for st in range(2):
            for d in range(2):
                copies[st][d][m].start()

    def carry1(a, k, copies):
        part, got = parts.at[k], recv1.at[a, k]
        for st in range(2):
            me = x if st == 0 else y
            for d in range(2):
                near = up(me) if d == 0 else down(me)
                lo = st * 16 + 8 * d
                copies[st][d][0].wait_recv()

                def trip(i, c, st=st, d=d, near=near, lo=lo):
                    for u in range(8):
                        there = got[st, d, 0, i, u].astype(F32)
                        if st == 0:
                            mine = part[i, near, lo + u].astype(F32)
                            part[i, near, lo + u] = (mine + there).astype(BF)
                        else:
                            mine = part[near, i, lo + u].astype(F32)
                            part[near, i, lo + u] = (mine + there).astype(BF)
                    return c

                lax.fori_loop(0, 4, trip, 0)
                copies[st][d][2].start()

    def close1(a, k, copies):
        part, got = parts.at[k], recv1.at[a, k]
        for m in (1, 2):
            for st in range(2):
                for d in range(2):
                    copies[st][d][m].wait_recv()
        for st in range(2):
            for h in range(2):
                lo = st * 16 + 8 * h

                def trip(i, c, st=st, h=h, lo=lo):
                    for u in range(8):
                        total = (
                            got[st, h, 2, i, u].astype(F32) + got[st, 1 - h, 1, i, u].astype(F32)
                        )
                        if st == 0:
                            part[i, x, lo + u] = (part[i, x, lo + u].astype(F32) + total).astype(BF)
                        else:
                            part[y, i, lo + u] = (part[y, i, lo + u].astype(F32) + total).astype(BF)
                    return c

                lax.fori_loop(0, 4, trip, 0)

    def carry2(a, k, copies):
        part, got = parts.at[k], recv2.at[a, k]
        for st in range(2):
            me = y if st == 0 else x
            for d in range(2):
                near = up(me) if d == 0 else down(me)
                lo = st * 16 + 8 * d
                copies[st][d][0].wait_recv()
                for u in range(8):
                    there = got[st, d, 0, u].astype(F32)
                    if st == 0:
                        part[near, x, lo + u] = (part[near, x, lo + u].astype(F32) + there).astype(BF)
                    else:
                        part[y, near, lo + u] = (part[y, near, lo + u].astype(F32) + there).astype(BF)
                copies[st][d][2].start()

    def close2(a, k, copies):
        part, got = parts.at[k], recv2.at[a, k]
        for m in (1, 2):
            for st in range(2):
                for d in range(2):
                    copies[st][d][m].wait_recv()
        for st in range(2):
            for h in range(2):
                for u in range(8):
                    b = st * 16 + 8 * h + u
                    total = (
                        part[y, x, b].astype(F32)
                        + got[st, h, 2, u].astype(F32)
                        + got[st, 1 - h, 1, u].astype(F32)
                    ).astype(BF)
                    outs[a][k, b] = total
                    if a == 0:
                        fields[1][k][row * OWN + b] = total

    def scatter_sent(*many):
        for copies in many:
            for st in range(2):
                for d in range(2):
                    for m in range(3):
                        copies[st][d][m].wait_send()

    for k in range(CHUNKS):
        for j in range(OWN):
            fields[0][k][row * OWN + j] = feat[k * CH:(k + 1) * CH, j * TILE:(j + 1) * TILE]
    runs[SLOTS] = jnp.zeros((CH, TILE), BF)

    items = [(a, k) for a in range(2) for k in range(CHUNKS)]
    total = len(items)
    g = [gather(a, k) for a, k in items]
    c1 = [scatter1(a, k) for a, k in items]
    c2 = [scatter2(a, k) for a, k in items]

    pl.semaphore_wait(barrier, 7)
    gather_start(g[0])
    gather_relay(g[0])
    gather_start(g[1])
    gather_share(g[0])

    for i in range(-1, total + 2):
        now, prev, old, nxt = i, i - 1, i - 2, i + 1
        is_now, is_prev, is_old = 0 <= now < total, 0 <= prev < total, 0 <= old < total
        is_next = nxt < total
        if is_prev:
            close1(*items[prev], c1[prev])
            start_messages(c2[prev], 0)
            start_messages(c2[prev], 1)
        if is_now:
            start_messages(c1[now], 1)
        if is_old:
            close2(*items[old], c2[old])
            if old < CHUNKS:
                gather_start(g[old + CHUNKS])
        if is_next:
            gather_finish(g[nxt])
            if nxt == 0:
                tile_copy.wait()
            acc = products(*items[nxt], 0, SLOTS // 2, zero())
        if is_now:
            carry1(*items[now], c1[now])
        if is_prev:
            carry2(*items[prev], c2[prev])
        if i + 2 < total:
            gather_relay(g[i + 2])
        if i + 3 < CHUNKS:
            gather_start(g[i + 3])
        if is_next:
            products(*items[nxt], SLOTS // 2, SLOTS, acc)
            if nxt >= CHUNKS:
                scatter_sent(c1[nxt - CHUNKS], c2[nxt - CHUNKS])
            pack(items[nxt][1])
            start_messages(c1[nxt], 0)
        if i + 2 < total:
            gather_share(g[i + 2])

    for i in range(total):
        gather_sent(g[i])
        if i >= CHUNKS:
            scatter_sent(c1[i], c2[i])


def combine_kernel(coef, feat, first, second, out):
    for k in range(CHUNKS):
        for j in range(OWN):
            nodes = slice(j * TILE, (j + 1) * TILE)
            base = feat[k * CH:(k + 1) * CH, nodes].astype(F32)
            one = first[k, j].astype(F32)
            two = 2.0 * second[k, j].astype(F32) - base
            for s in range(SCALES):
                value = coef[0, s] * base + coef[1, s] * one + coef[2, s] * two
                out[s * CHANNELS + k * CH:s * CHANNELS + (k + 1) * CH, nodes] = value.astype(BF)


def shards(features, tile_rows, tile_cols, tile_count, tile_data):
    perm, cols, keep, last = slot_tables(
        tile_rows.reshape(-1), tile_cols.reshape(-1), tile_count.reshape(())
    )
    smem = pl.BlockSpec(memory_space=pltpu.SMEM)
    vmem = pl.BlockSpec(memory_space=pltpu.VMEM)
    half = jax.ShapeDtypeStruct((CHUNKS, OWN, CH, TILE), BF)
    field = pltpu.VMEM((8 * OWN, CH, TILE), BF)
    part = pltpu.VMEM((CHUNKS, 4, 4, OWN, CH, TILE), BF)
    got1 = pltpu.VMEM((2, CHUNKS, 2, 2, 3, 4, 8, CH, TILE), BF)
    got2 = pltpu.VMEM((2, CHUNKS, 2, 2, 3, 8, CH, TILE), BF)
    dma = pltpu.SemaphoreType.DMA
    first, second = pl.pallas_call(
        chain_kernel,
        out_shape=(half, half),
        in_specs=[smem, smem, smem, smem, vmem, pl.BlockSpec(memory_space=pl.ANY)],
        out_specs=(vmem, vmem),
        scratch_shapes=[
            pltpu.VMEM((SLOTS, TILE, TILE), BF),
            field, field, field, field, field, field, field, field,
            pltpu.VMEM((SLOTS + 1, CH, TILE), BF),
            part, got1, got2,
            dma,
            dma((2, CHUNKS, 2, 2, 3)), dma((2, CHUNKS, 2, 2, 3)),
            dma((2, CHUNKS, 2, 2, 3)), dma((2, CHUNKS, 2, 2, 3)),
            dma((2, CHUNKS, 13)), dma((2, CHUNKS, 13)),
        ],
        compiler_params=pltpu.CompilerParams(
            collective_id=0, has_side_effects=True, vmem_limit_bytes=62 * 1024 * 1024
        ),
        name="chain",
    )(perm, cols, keep, last, features, tile_data.reshape(SLOTS, TILE, TILE))

    coef = jnp.stack(coefficients())
    return pl.pallas_call(
        combine_kernel,
        out_shape=jax.ShapeDtypeStruct((SCALES * CHANNELS, OWN * TILE), BF),
        in_specs=[smem, vmem, vmem, vmem],
        out_specs=vmem,
        name="combine",
    )(coef, features, first, second)


def solution(mesh):
    return jax.shard_map(
        shards,
        mesh=mesh,
        in_specs=(
            P(None, ("row", "col")),
            P("row", "col", None),
            P("row", "col", None),
            P("row", "col"),
            P("row", "col", None, None, None),
        ),
        out_specs=P(None, ("row", "col")),
        check_vma=False,
    )
```

```python
import functools

import jax
import jax.numpy as jnp
import numpy as np
from jax import lax
from jax.experimental import pallas as pl
from jax.experimental.pallas import tpu as pltpu
from jax.sharding import PartitionSpec as P

TILE = 128
SLOTS = 512
CHANNELS = 64
CHUNKS = 4
CH = CHANNELS // CHUNKS
SCALES = 8
OWN = 32
UNROLL = 64
PIECES = 8
MESH = pl.DeviceIdType.MESH
BF = jnp.bfloat16
F32 = jnp.float32


def bessel_pair(times):
    halved = times / np.float32(2.0)
    square = halved * halved
    term_zero = np.ones_like(times)
    term_one = halved
    sum_zero = term_zero
    sum_one = term_one
    for degree in range(1, 24):
        term_zero = term_zero * square / np.float32(degree * degree)
        term_one = term_one * square / np.float32(degree * (degree + 1))
        sum_zero = sum_zero + term_zero
        sum_one = sum_one + term_one
    damping = np.exp(-times)
    return (damping * sum_zero, damping * sum_one)


def coefficients():
    two = np.float32(2.0)
    times = np.float32(0.25) * two ** (np.arange(SCALES).astype(np.float32) / two)
    bessel_zero, bessel_one = bessel_pair(times.astype(np.float32))
    return (bessel_zero, -two * bessel_one, two * (bessel_zero - two * bessel_one / times))


def flipped(line):
    return jnp.broadcast_to(line, (TILE, TILE)).T


def slot_tables(live, slot_rows, slot_cols, ints, floats):
    live_count = live[0, 0]
    lanes = lax.broadcasted_iota(jnp.int32, (1, TILE), 1)
    deep = lax.broadcasted_iota(jnp.int32, (TILE, TILE), 0).astype(F32)
    groups = SLOTS // TILE
    keys, rows_t, keys_t, pairs_t = [], [], [], []
    for j in range(groups):
        span = slice(j * TILE, (j + 1) * TILE)
        ids = lanes + j * TILE
        rows = jnp.where(ids < live_count, slot_rows[0, :, span], SLOTS).astype(F32)
        keys.append(rows * SLOTS + ids.astype(F32))
        rows_t.append(flipped(rows))
        keys_t.append(flipped(keys[j]))
        pairs_t.append(rows_t[j] * 256.0 + flipped(slot_cols[0, :, span].astype(F32)))

    def count(masks):
        total = jnp.zeros((TILE, TILE), F32)
        for mask in masks:
            total = total + mask
        return jnp.sum(total, axis=0, keepdims=True)

    ranks_t = [
        flipped(count(jnp.where(keys_t[i] < keys[j], 1.0, 0.0) for i in range(groups)))
        for j in range(groups)
    ]
    ints[3 * groups:] = jnp.zeros((4, TILE), jnp.int32)
    floats[groups:] = jnp.zeros((4, TILE), F32)
    for j in range(groups):
        place = (lanes + j * TILE).astype(F32)
        perm = count(jnp.where(ranks_t[i] == place, deep + float(i * TILE), 0.0) for i in range(groups))
        pair = count(jnp.where(ranks_t[i] == place, pairs_t[i], 0.0) for i in range(groups))
        before = count(jnp.where(ranks_t[i] == place - 1.0, rows_t[i], 0.0) for i in range(groups))
        upto = count(jnp.where(rows_t[i] <= place, 1.0, 0.0) for i in range(groups))
        here = count(jnp.where(rows_t[i] == place, 1.0, 0.0) for i in range(groups))
        pair = pair.astype(jnp.int32)
        rows = pair // 256
        ints[j:j + 1] = perm.astype(jnp.int32)
        ints[groups + j:groups + j + 1] = pair - rows * 256
        ints[2 * groups + j:2 * groups + j + 1] = jnp.where(here > 0.0, upto - 1.0, float(SLOTS)).astype(jnp.int32)
        floats[j:j + 1] = jnp.where(rows.astype(F32) == before, 1.0, 0.0)


def chain_kernel(
    table, keep, feat_hbm, tdata, first_out, second_out,
    tiles, f00, f01, f02, f03, f10, f11, f12, f13, runs, parts, recv1, recv2,
    feat, finals,
    tile_sem, feat_sem, out_sem, s1, v1, s2, v2, sa, va, sf, vf,
):
    row = lax.axis_index("row")
    col = lax.axis_index("col")
    z, core = row // 2, row % 2
    y, x = col // 4, col % 4
    fields = ((f00, f01, f02, f03), (f10, f11, f12, f13))
    outs = (first_out, second_out)

    def up(v):
        return (v + 1) % 4

    def down(v):
        return (v + 3) % 4

    def far(v):
        return (v + 2) % 4

    z_next = (up(z) * 2 + core, col)
    z_prev = (down(z) * 2 + core, col)
    mate = (z * 2 + (1 - core), col)
    x_next = (row, y * 4 + up(x))
    x_prev = (row, y * 4 + down(x))
    y_next = (row, up(y) * 4 + x)
    y_prev = (row, down(y) * 4 + x)

    barrier = pltpu.get_barrier_semaphore()
    for other in (z_next, z_prev, mate, x_next, x_prev, y_next, y_prev):
        pl.semaphore_signal(barrier, inc=1, device_id=other, device_id_type=MESH)

    feat_copies = [
        pltpu.make_async_copy(
            feat_hbm.at[pl.ds(k * CH, CH)], feat.at[pl.ds(k * CH, CH)], feat_sem.at[k]
        )
        for k in range(CHUNKS)
    ]
    for c in feat_copies:
        c.start()

    piece = SLOTS // PIECES
    tile_copies = [
        pltpu.make_async_copy(
            tdata.at[pl.ds(n * piece, piece)], tiles.at[pl.ds(n * piece, piece)], tile_sem.at[n]
        )
        for n in range(PIECES)
    ]
    for c in tile_copies:
        c.start()

    def turn(n):
        tile_copies[n].wait()

        def trip(i, carry):
            for u in range(8):
                t = n * piece + i * 8 + u
                tiles[t] = tiles[t].T
            return carry

        lax.fori_loop(0, piece // 8, trip, 0)

    def send(src, dst, ssem, rsem, to):
        return pltpu.make_async_remote_copy(
            src_ref=src, dst_ref=dst, send_sem=ssem, recv_sem=rsem,
            device_id=to, device_id_type=MESH,
        )

    def gather(a, k):
        ref = fields[a][k]
        half = OWN // 2

        def block(zz, h=None):
            start = (zz * 2 + core) * OWN
            if h is None:
                return ref.at[pl.ds(start, OWN)]
            return ref.at[pl.ds(start + h * half, half)]

        def copy(i, view, to):
            return send(view, view, sa.at[a, k, i], va.at[a, k, i], to)

        zp, zn, zf = down(z), up(z), far(z)
        return [
            copy(0, block(z, 0), z_next),
            copy(1, block(z, 1), z_next),
            copy(2, block(z, 0), z_prev),
            copy(3, block(z, 1), z_prev),
            copy(4, block(zp, 0), z_next),
            copy(5, block(zn, 1), z_prev),
            copy(6, block(z), mate),
            copy(7, block(zp, 0), mate),
            copy(8, block(zp, 1), mate),
            copy(9, block(zn, 0), mate),
            copy(10, block(zn, 1), mate),
            copy(11, block(zf, 0), mate),
            copy(12, block(zf, 1), mate),
        ]

    def gather_start(g):
        g[0].start()
        g[3].start()
        g[1].start()
        g[2].start()
        g[6].start()

    def gather_relay(g):
        g[0].wait_recv()
        g[4].start()
        g[7].start()
        g[3].wait_recv()
        g[5].start()
        g[10].start()

    def gather_share(g):
        g[1].wait_recv()
        g[8].start()
        g[2].wait_recv()
        g[9].start()
        g[4].wait_recv()
        g[11].start()
        g[5].wait_recv()
        g[12].start()

    def gather_finish(g):
        for i in range(6, 13):
            g[i].wait_recv()

    def gather_sent(g):
        for c in g:
            c.wait_send()

    def products(a, k, begin, end, acc):
        field = fields[a][k]

        def trip(i, acc):
            line, at = i // 2, (i % 2) * UNROLL
            for u in range(0, UNROLL, 2):
                s = i * UNROLL + u
                lhs = jnp.concatenate([
                    field[table[4 + line, at + u]], field[table[4 + line, at + u + 1]]
                ], axis=0)
                rhs = jnp.concatenate([
                    tiles[table[line, at + u]], tiles[table[line, at + u + 1]]
                ], axis=1)
                pair = jnp.dot(lhs, rhs, preferred_element_type=F32)
                acc = acc * keep[line, at + u] + pair[:CH, :TILE]
                runs[s] = acc.astype(BF)
                acc = acc * keep[line, at + u + 1] + pair[CH:, TILE:]
                runs[s + 1] = acc.astype(BF)
            return acc

        return lax.fori_loop(begin // UNROLL, end // UNROLL, trip, acc)

    def zero():
        return jnp.zeros((CH, TILE), F32)

    def pack(k):
        part = parts.at[k]

        def trip(i, carry):
            for xx in range(4):
                for u in range(8):
                    part[i // 4, xx, (i % 4) * 8 + u] = runs[table[8 + i // 4, xx * 32 + (i % 4) * 8 + u]]
            return carry

        lax.fori_loop(0, 16, trip, 0)

    def scatter1(a, k):
        part, got = parts.at[k], recv1.at[a, k]
        out = []
        for st in range(2):
            base = st * 16
            me = x if st == 0 else y
            nxt = x_next if st == 0 else y_next
            prv = x_prev if st == 0 else y_prev

            def view(who, h, st=st, base=base):
                if st == 0:
                    return part.at[:, who, pl.ds(base + 8 * h, 8)]
                return part.at[who, :, pl.ds(base + 8 * h, 8)]

            rows = []
            for d in range(2):
                to = nxt if d == 0 else prv
                near = up(me) if d == 0 else down(me)
                views = (view(far(me), d), view(near, 1 - d), view(near, d))
                rows.append([
                    send(views[m], got.at[st, d, m], s1.at[a, k, st, d, m], v1.at[a, k, st, d, m], to)
                    for m in range(3)
                ])
            out.append(rows)
        return out

    def scatter2(a, k):
        part, got = parts.at[k], recv2.at[a, k]
        out = []
        for st in range(2):
            base = st * 16
            me = y if st == 0 else x
            nxt = y_next if st == 0 else x_next
            prv = y_prev if st == 0 else x_prev

            def view(who, h, st=st, base=base):
                if st == 0:
                    return part.at[who, x, pl.ds(base + 8 * h, 8)]
                return part.at[y, who, pl.ds(base + 8 * h, 8)]

            rows = []
            for d in range(2):
                to = nxt if d == 0 else prv
                near = up(me) if d == 0 else down(me)
                views = (view(far(me), d), view(near, 1 - d), view(near, d))
                rows.append([
                    send(views[m], got.at[st, d, m], s2.at[a, k, st, d, m], v2.at[a, k, st, d, m], to)
                    for m in range(3)
                ])
            out.append(rows)
        return out

    def start_messages(copies, m):
        for st in range(2):
            for d in range(2):
                copies[st][d][m].start()

    def carry1(a, k, copies):
        part, got = parts.at[k], recv1.at[a, k]
        for st in range(2):
            me = x if st == 0 else y
            for d in range(2):
                near = up(me) if d == 0 else down(me)
                lo = st * 16 + 8 * d
                copies[st][d][0].wait_recv()

                def trip(i, c, st=st, d=d, near=near, lo=lo):
                    for u in range(8):
                        there = got[st, d, 0, i, u].astype(F32)
                        if st == 0:
                            mine = part[i, near, lo + u].astype(F32)
                            part[i, near, lo + u] = (mine + there).astype(BF)
                        else:
                            mine = part[near, i, lo + u].astype(F32)
                            part[near, i, lo + u] = (mine + there).astype(BF)
                    return c

                lax.fori_loop(0, 4, trip, 0)
                copies[st][d][2].start()

    def close1(a, k, copies):
        part, got = parts.at[k], recv1.at[a, k]
        for m in (1, 2):
            for st in range(2):
                for d in range(2):
                    copies[st][d][m].wait_recv()
        for st in range(2):
            for h in range(2):
                lo = st * 16 + 8 * h

                def trip(i, c, st=st, h=h, lo=lo):
                    for u in range(8):
                        total = (
                            got[st, h, 2, i, u].astype(F32) + got[st, 1 - h, 1, i, u].astype(F32)
                        )
                        if st == 0:
                            part[i, x, lo + u] = (part[i, x, lo + u].astype(F32) + total).astype(BF)
                        else:
                            part[y, i, lo + u] = (part[y, i, lo + u].astype(F32) + total).astype(BF)
                    return c

                lax.fori_loop(0, 4, trip, 0)

    def order(st):
        me = y if st == 0 else x
        return (far(me), up(me), down(me), me)

    def scatter1_fine(a, k):
        part, got = parts.at[k], recv1.at[a, k]
        out = []
        for st in range(2):
            me = x if st == 0 else y
            rows = []
            for d in range(2):
                near = up(me) if d == 0 else down(me)
                if st == 0:
                    to = x_next if d == 0 else x_prev
                else:
                    to = y_next if d == 0 else y_prev
                line = []
                for n, o in enumerate(order(st)):
                    where = (o, near) if st == 0 else (near, o)
                    line.append(send(
                        part.at[where[0], where[1], pl.ds(st * 16 + 8 * d, 8)], got.at[st, d, 2, o],
                        sf.at[st, d, n], vf.at[st, d, n], to,
                    ))
                rows.append(line)
            out.append(rows)
        return out

    def carry1_fine(a, k, copies, fine):
        part, got = parts.at[k], recv1.at[a, k]
        for st in range(2):
            for d in range(2):
                copies[st][d][0].wait_recv()
        for n in range(4):
            for st in range(2):
                me = x if st == 0 else y
                o = order(st)[n]
                for d in range(2):
                    near = up(me) if d == 0 else down(me)
                    p, q = (o, near) if st == 0 else (near, o)
                    for u in range(8):
                        b = st * 16 + 8 * d + u
                        part[p, q, b] = (
                            part[p, q, b].astype(F32) + got[st, d, 0, o, u].astype(F32)
                        ).astype(BF)
                    fine[st][d][n].start()

    def close1_fine(a, k, copies, fine, later):
        part, got = parts.at[k], recv1.at[a, k]
        for st in range(2):
            for d in range(2):
                copies[st][d][1].wait_recv()
        for n in range(4):
            for st in range(2):
                o = order(st)[n]
                for d in range(2):
                    fine[st][d][n].wait_recv()
                p, q = (o, x) if st == 0 else (y, o)
                for h in range(2):
                    for u in range(8):
                        b = st * 16 + 8 * h + u
                        part[p, q, b] = (
                            part[p, q, b].astype(F32)
                            + got[st, h, 2, o, u].astype(F32)
                            + got[st, 1 - h, 1, o, u].astype(F32)
                        ).astype(BF)
                if n == 0:
                    later[st][0][0].start()
                    later[st][1][0].start()
                elif n < 3:
                    later[st][n - 1][1].start()

    def carry2(a, k, copies):
        part, got = parts.at[k], recv2.at[a, k]
        for st in range(2):
            me = y if st == 0 else x
            for d in range(2):
                near = up(me) if d == 0 else down(me)
                lo = st * 16 + 8 * d
                copies[st][d][0].wait_recv()
                for u in range(8):
                    there = got[st, d, 0, u].astype(F32)
                    if st == 0:
                        part[near, x, lo + u] = (part[near, x, lo + u].astype(F32) + there).astype(BF)
                    else:
                        part[y, near, lo + u] = (part[y, near, lo + u].astype(F32) + there).astype(BF)
                copies[st][d][2].start()

    def close2(a, k, copies):
        part, got = parts.at[k], recv2.at[a, k]
        for m in (1, 2):
            for st in range(2):
                for d in range(2):
                    copies[st][d][m].wait_recv()
        for st in range(2):
            for h in range(2):
                for u in range(8):
                    b = st * 16 + 8 * h + u
                    total = (
                        part[y, x, b].astype(F32)
                        + got[st, h, 2, u].astype(F32)
                        + got[st, 1 - h, 1, u].astype(F32)
                    ).astype(BF)
                    if a == 0:
                        fields[1][k][row * OWN + b] = total
                    else:
                        finals[k, b] = total

    def deliver(a, k):
        source = fields[1][k].at[pl.ds(row * OWN, OWN)] if a == 0 else finals.at[k]
        return pltpu.make_async_copy(source, outs[a].at[k], out_sem.at[a, k])

    def scatter_sent(*many):
        for copies in many:
            for st in range(2):
                for d in range(2):
                    for m in range(3):
                        copies[st][d][m].wait_send()

    def own(k):
        feat_copies[k].wait()
        for j in range(OWN):
            fields[0][k][row * OWN + j] = feat[k * CH:(k + 1) * CH, j * TILE:(j + 1) * TILE]

    items = [(a, k) for a in range(2) for k in range(CHUNKS)]
    total = len(items)
    g = [gather(a, k) for a, k in items]
    c1 = [scatter1(a, k) for a, k in items]
    c2 = [scatter2(a, k) for a, k in items]
    deliveries = [deliver(a, k) for a, k in items]
    fine = scatter1_fine(*items[-1])

    own(0)
    pl.semaphore_wait(barrier, 7)
    gather_start(g[0])
    for k in range(1, CHUNKS):
        own(k)
    runs[SLOTS] = jnp.zeros((CH, TILE), BF)
    turn(0)
    turn(1)
    gather_relay(g[0])
    gather_start(g[1])
    for n in range(2, 5):
        turn(n)
    gather_share(g[0])
    for n in range(5, PIECES):
        turn(n)

    for i in range(-1, total):
        now, prev, old, nxt = i, i - 1, i - 2, i + 1
        is_now, is_prev, is_old = 0 <= now < total, 0 <= prev < total, 0 <= old < total
        is_next = nxt < total
        if is_prev:
            close1(*items[prev], c1[prev])
            start_messages(c2[prev], 0)
            start_messages(c2[prev], 1)
        if is_now:
            start_messages(c1[now], 1)
        if is_old:
            close2(*items[old], c2[old])
            deliveries[old].start()
            if old < CHUNKS:
                gather_start(g[old + CHUNKS])
        if is_next:
            gather_finish(g[nxt])
            acc = products(*items[nxt], 0, SLOTS // 2, zero())
        if now == total - 1:
            carry2(*items[prev], c2[prev])
            carry1_fine(*items[now], c1[now], fine)
        else:
            if is_now:
                carry1(*items[now], c1[now])
            if is_prev:
                carry2(*items[prev], c2[prev])
        if i + 2 < total:
            gather_relay(g[i + 2])
        if i + 3 < CHUNKS:
            gather_start(g[i + 3])
        if is_next:
            products(*items[nxt], SLOTS // 2, SLOTS, acc)
            if nxt >= CHUNKS:
                scatter_sent(c1[nxt - CHUNKS], c2[nxt - CHUNKS])
            pack(items[nxt][1])
            start_messages(c1[nxt], 0)
        if i + 2 < total:
            gather_share(g[i + 2])

    close1_fine(*items[-1], c1[-1], fine, c2[-1])
    carry2(*items[-1], c2[-1])
    close2(*items[-2], c2[-2])
    deliveries[-2].start()
    close2(*items[-1], c2[-1])
    deliveries[-1].start()

    for i in range(total):
        gather_sent(g[i])
        if i == total - 1:
            for st in range(2):
                for d in range(2):
                    for m in range(2):
                        c1[i][st][d][m].wait_send()
                    for c in fine[st][d]:
                        c.wait_send()
            scatter_sent(c2[i])
        elif i >= CHUNKS:
            scatter_sent(c1[i], c2[i])
        deliveries[i].wait()


def combine_kernel(coef, feat, first, second, out, stage, sem):
    copies = []
    for k in range(CHUNKS):
        channels = slice(k * CH, (k + 1) * CH)
        for j in range(OWN):
            nodes = slice(j * TILE, (j + 1) * TILE)
            base = feat[channels, nodes].astype(F32)
            one = first[k, j].astype(F32)
            two = 2.0 * second[k, j].astype(F32) - base
            for s in range(SCALES):
                value = coef[0][s] * base + coef[1][s] * one + coef[2][s] * two
                stage[s * CHANNELS + k * CH:s * CHANNELS + (k + 1) * CH, nodes] = value.astype(BF)
        for s in range(SCALES):
            block = pl.ds(s * CHANNELS + k * CH, CH)
            copies.append(pltpu.make_async_copy(stage.at[block], out.at[block], sem.at[k, s]))
            copies[-1].start()
    for c in copies:
        c.wait()


def shards(features, tile_rows, tile_cols, tile_count, tile_data):
    smem = pl.BlockSpec(memory_space=pltpu.SMEM)
    vmem = pl.BlockSpec(memory_space=pltpu.VMEM)
    hbm = pl.BlockSpec(memory_space=pl.ANY)
    half = jax.ShapeDtypeStruct((CHUNKS, OWN, CH, TILE), BF)
    field = pltpu.VMEM((8 * OWN, CH, TILE), BF)
    part = pltpu.VMEM((CHUNKS, 4, 4, OWN, CH, TILE), BF)
    got1 = pltpu.VMEM((2, CHUNKS, 2, 2, 3, 4, 8, CH, TILE), BF)
    got2 = pltpu.VMEM((2, CHUNKS, 2, 2, 3, 8, CH, TILE), BF)
    dma = pltpu.SemaphoreType.DMA
    table, keep = pl.pallas_call(
        slot_tables,
        out_shape=(
            jax.ShapeDtypeStruct((16, TILE), jnp.int32), jax.ShapeDtypeStruct((8, TILE), F32)
        ),
        in_specs=[smem, vmem, vmem],
        out_specs=(vmem, vmem),
        name="tables",
    )(tile_count, tile_rows, tile_cols)
    first, second = pl.pallas_call(
        chain_kernel,
        out_shape=(half, half),
        in_specs=[smem, smem, hbm, hbm],
        out_specs=(hbm, hbm),
        scratch_shapes=[
            pltpu.VMEM((SLOTS, TILE, TILE), BF),
            field, field, field, field, field, field, field, field,
            pltpu.VMEM((SLOTS + 1, CH, TILE), BF),
            part, got1, got2,
            pltpu.VMEM((CHANNELS, OWN * TILE), BF), pltpu.VMEM((CHUNKS, OWN, CH, TILE), BF),
            dma((PIECES,)), dma((CHUNKS,)), dma((2, CHUNKS)),
            dma((2, CHUNKS, 2, 2, 3)), dma((2, CHUNKS, 2, 2, 3)),
            dma((2, CHUNKS, 2, 2, 3)), dma((2, CHUNKS, 2, 2, 3)),
            dma((2, CHUNKS, 13)), dma((2, CHUNKS, 13)),
            dma((2, 2, 4)), dma((2, 2, 4)),
        ],
        compiler_params=pltpu.CompilerParams(
            collective_id=0, has_side_effects=True, vmem_limit_bytes=62 * 1024 * 1024
        ),
        name="chain",
    )(table, keep, features, tile_data.reshape(SLOTS, TILE, TILE))

    coef = [[float(value) for value in line] for line in coefficients()]
    return pl.pallas_call(
        functools.partial(combine_kernel, coef),
        out_shape=jax.ShapeDtypeStruct((SCALES * CHANNELS, OWN * TILE), BF),
        in_specs=[vmem, vmem, vmem],
        out_specs=hbm,
        scratch_shapes=[
            pltpu.VMEM((SCALES * CHANNELS, OWN * TILE), BF),
            dma((CHUNKS, SCALES)),
        ],
        name="combine",
    )(features, first, second)


def solution(mesh):
    return jax.shard_map(
        shards,
        mesh=mesh,
        in_specs=(
            P(None, ("row", "col")),
            P("row", "col", None),
            P("row", "col", None),
            P("row", "col"),
            P("row", "col", None, None, None),
        ),
        out_specs=P(None, ("row", "col")),
        check_vma=False,
    )
```
